32 devices in a mesh: section: 2 (over x), expert: 4 (over y, core), dp: 4 (over z).
Axes of the slice: x: 2, y: 2, z: 4, core: 2. Of those that a mesh axis runs over, the one named last changes fastest.
Arguments:
- x_in: bfloat16 [8, 256, 2048], P(None, ('expert', 'dp'), 'section'), may hold values from -6 to 6
- cotangent: bfloat16 [8, 256, 2048], P(None, ('expert', 'dp'), 'section'), may hold values from -6 to 6
- route_ids: int32 [2, 8, 256, 2], P('section', None, ('expert', 'dp')), may hold values from 0 to 15, all different within a row; in each aligned block of 16 rows (0 to 15, 16 to 31, ..., all dimensions but the last counted through in order) at most 2 rows name the same one
- norm_gain: float32 [2, 2048], P('section'), may hold values from 0.5 to 1.5
- router: bfloat16 [2, 2048, 16], P('section'), may hold values from -0.125 to 0.125
- w_gate_up: bfloat16 [2, 16, 2048, 1024], P('section', ('expert', 'dp')), may hold values from -0.125 to 0.125
- w_down: bfloat16 [2, 16, 512, 2048], P('section', ('expert', 'dp')), may hold values from -0.25 to 0.25
Outputs:
- grad_in: bfloat16 [8, 256, 2048], P(None, ('expert', 'dp'), 'section')
- grad_gate_up: float32 [2, 16, 2048, 1024], P('section', ('expert', 'dp'))
- grad_down: float32 [2, 16, 512, 2048], P('section', ('expert', 'dp'))
- grad_router: float32 [2, 2048, 16], P('section')
- grad_gain: float32 [2, 2048], P('section')
The draws below stay inside these ranges and needn't reach their ends.
Inputs may be any that keep to these rules, and one draw needn't show every extreme that they name: `route_ids`: each row names two different experts; the 16 rows of one device in one layer and micro-batch name any expert at most 2 times, a bound that some block reaches in some of them.
All inputs are finite; a program needn't handle non-finite values.
Results may differ from the reference program's by a relative error of at most 0.035.
Values may be sent and summed in bfloat16 or wider, within the bound.
A program may use at most 64 MiB of HBM per device.

```python
import math
import jax
import jax.numpy as jnp
import numpy as np
from jax import lax

D = 2048
FFW = 512
TOP = 2
MICRO = 8
TOK_DEV = 16
EXPERTS = 16
CAP = 2
ROWS = 256
SECTIONS = 2


def shard_levels(own_key, shape, pieces, low, high):
    def one(axis_at, blocks):
        heights = jax.random.uniform(jax.random.fold_in(jax.random.fold_in(own_key, 6), axis_at), (blocks,), jnp.float32, low / len(pieces), high / len(pieces))
        return jnp.repeat(jnp.exp(heights), shape[axis_at] // blocks).reshape((-1,) + (1,) * (len(shape) - axis_at - 1))

    level = one(*pieces[0])
    for cut in pieces[1:]:
        level = level * one(*cut)
    return level


def routed_block(key, own, number, rows, count, top, reach, lean):
    sequence = jax.random.permutation(key, count)
    packed, ordinary = shares(count, rows * top, reach, lean, True), shares(count, rows * top, reach, lean, False)
    places = jnp.arange(count)

    def named(lengths, turn):
        used = int((lengths > 0).sum())
        fixed = max(1, used // 4)
        moved = fixed + (places - fixed + turn * (used - fixed)) % max(1, count - fixed)
        return jnp.zeros((count,), jnp.int32).at[sequence[jnp.where(places < fixed, places, moved)]].set(jnp.asarray(lengths, jnp.int32))

    lengths = jnp.where(number % 4 == 0, named(packed, number // 4), named(ordinary, number - number // 4 - 1))
    mixed = jax.random.permutation(jax.random.fold_in(own, 3), count)
    donor, taker = mixed[0:count // 2 * 2:2], mixed[1:count // 2 * 2:2]
    slack = jnp.minimum(lengths[donor] - 1, reach - lengths[taker]) // 2
    slack = jnp.where((donor == sequence[0]) | (taker == sequence[0]) | (lengths[taker] == 0), 0, jnp.maximum(slack, 0))
    moved = jax.random.randint(jax.random.fold_in(own, 4), (count // 2,), 0, 1 << 20) % (slack + 1)
    lengths = lengths.at[donor].add(-moved).at[taker].add(moved)
    items = jnp.searchsorted(jnp.cumsum(lengths), jnp.arange(rows * top), side="right").astype(jnp.int32)
    listing = items.reshape(top, rows).T
    listing = listing[jax.random.permutation(jax.random.fold_in(own, 1), rows)]
    turn = jax.random.randint(jax.random.fold_in(own, 2), (rows, 1), 0, top)
    return jnp.take_along_axis(listing, (jnp.arange(top)[None, :] + turn) % top, axis=1)


def shares(count, total, bound, slope, full):
    portions = [(1 << 20) // math.isqrt(rank ** slope) + 1 for rank in range(1, count + 1)]
    largest = bound if full else min(bound, max(-(-total // count), total * portions[0] // sum(portions)))
    least = 1 if total - largest >= count - 1 else 0
    holding, rest = [largest] + [least] * (count - 1), total - largest - least * (count - 1)
    while rest > 0:
        candidates = [i for i in range(1, count) if holding[i] < largest] or [i for i in range(1, count) if holding[i] < bound]
        mass, budget = sum([portions[i] for i in candidates]), rest
        for i in candidates:
            addition = min(bound - holding[i], max(1, budget * portions[i] // mass), rest)
            holding[i] = holding[i] + addition
            rest = rest - addition
    return np.array(holding)


def gaussian(stream_key, dims, width, limit, shards=(), kind=jnp.bfloat16):
    array = jax.random.normal(stream_key, dims, jnp.float32) * width
    if len(shards) > 0:
        array = shard_levels(stream_key, dims, shards, -0.22, 0.18) * array
    return jnp.clip(array, min=-limit, max=limit).astype(kind)


def setup_inputs(seed: int = 0) -> dict:
    arg_keys = jax.random.split(jax.random.key(seed), 8)
    x_in = gaussian(arg_keys[0], (MICRO, ROWS, D), 1.0, 6.0, ((1, 16), (2, 2)))
    cotangent = gaussian(arg_keys[1], (MICRO, ROWS, D), 1.0, 6.0, ((1, 16), (2, 2)))
    route_ids_keys = jax.random.split(jax.random.fold_in(arg_keys[2], 1), SECTIONS * MICRO * ROWS // TOK_DEV)
    route_ids_turns = jax.random.permutation(jax.random.fold_in(arg_keys[2], 3), SECTIONS * MICRO * ROWS // TOK_DEV)
    route_ids = jax.vmap(lambda own, number: routed_block(jax.random.fold_in(arg_keys[2], 2), own, number, TOK_DEV, EXPERTS, TOP, CAP, 2))(route_ids_keys, route_ids_turns).reshape((SECTIONS, MICRO, ROWS, TOP))
    norm_gain = jnp.clip(1.0 + 0.1 * jax.random.normal(arg_keys[3], (SECTIONS, D), jnp.float32), 0.5, 1.5)
    router = gaussian(arg_keys[4], (SECTIONS, D, EXPERTS), D ** -0.5, 0.125, ((0, 2),))
    w_gate_up = gaussian(arg_keys[5], (SECTIONS, EXPERTS, D, 2 * FFW), D ** -0.5, 0.125, ((0, 2), (1, 16)))
    w_down = gaussian(arg_keys[6], (SECTIONS, EXPERTS, FFW, D), FFW ** -0.5, 0.25, ((0, 2), (1, 16)))
    return dict(x_in=x_in, cotangent=cotangent, route_ids=route_ids, norm_gain=norm_gain, router=router, w_gate_up=w_gate_up, w_down=w_down)


EPS = 1e-05

def rounded(value):
    return lax.optimization_barrier(value.astype(jnp.bfloat16))

def slot_tables(route_rows):
    experts = jnp.arange(EXPERTS, dtype=jnp.int32)
    expert_hits = (route_rows[..., None] == experts).astype(jnp.int32)
    per_expert = lax.optimization_barrier(jnp.sum(expert_hits, axis=-2))
    before = jnp.cumsum(per_expert, axis=-2) - per_expert
    slot_ids = lax.optimization_barrier(jnp.sum(expert_hits * before[..., None, :], axis=-1))
    dest_cell = route_rows * CAP + slot_ids
    cell_ids = jnp.arange(EXPERTS * CAP, dtype=jnp.int32)
    slot_place = (dest_cell[..., None] == cell_ids).astype(jnp.float32)
    return (expert_hits.astype(jnp.float32), slot_place)

def layer_state(layer_in, route_rows, gain_vec, router_mat, w_gu):
    blocks = ROWS // TOK_DEV
    h_wide = layer_in.reshape(MICRO, blocks, TOK_DEV, D).astype(jnp.float32)
    inv_rms = lax.rsqrt(lax.optimization_barrier(jnp.mean(h_wide * h_wide, axis=-1, keepdims=True)) + EPS)
    normed = rounded(h_wide * inv_rms * gain_vec).astype(jnp.float32)
    expert_hits, slot_place = slot_tables(route_rows.reshape(MICRO, blocks, TOK_DEV, TOP))
    logits = jnp.einsum('mbtd,de->mbte', normed, router_mat.astype(jnp.float32), precision=lax.Precision.HIGHEST)
    chosen = lax.optimization_barrier(jnp.sum(expert_hits * logits[..., None, :], axis=-1))
    first_gate = jax.nn.sigmoid(chosen[..., 0] - chosen[..., 1])
    second_gate = jax.nn.sigmoid(chosen[..., 1] - chosen[..., 0])
    exp_rows = rounded(jnp.einsum('mbtkc,mbtd->mbcd', slot_place, normed, precision=lax.Precision.HIGHEST))
    exp_rows = exp_rows.astype(jnp.float32).reshape(MICRO, blocks, EXPERTS, CAP, D)
    gate_up = jnp.einsum('mbecd,edf->mbecf', exp_rows, w_gu.astype(jnp.float32), precision=lax.Precision.HIGHEST)
    gate_part = gate_up[..., :FFW]
    up_part = gate_up[..., FFW:]
    sigmoid_gate = jax.nn.sigmoid(gate_part)
    hidden = rounded(gate_part * sigmoid_gate * up_part).astype(jnp.float32)
    return (h_wide, inv_rms, normed, expert_hits, slot_place, first_gate, second_gate, exp_rows, gate_part, up_part, sigmoid_gate, hidden)

def expert_out(hidden, w_dn):
    blocks = ROWS // TOK_DEV
    out_rows = rounded(jnp.einsum('mbecf,efd->mbecd', hidden, w_dn.astype(jnp.float32), precision=lax.Precision.HIGHEST))
    return out_rows.astype(jnp.float32).reshape(MICRO, blocks, EXPERTS * CAP, D)

def forward_layer(layer_in, route_rows, gain_vec, router_mat, w_gu, w_dn):
    state = layer_state(layer_in, route_rows, gain_vec, router_mat, w_gu)
    h_wide, slot_place, first_gate, second_gate, hidden = (state[0], state[4], state[5], state[6], state[11])
    picked = jnp.einsum('mbtkc,mbcd->mbtkd', slot_place, expert_out(hidden, w_dn), precision=lax.Precision.HIGHEST)
    layer_out = h_wide + first_gate[..., None] * picked[..., 0, :] + second_gate[..., None] * picked[..., 1, :]
    return layer_out.astype(jnp.bfloat16).reshape(MICRO, ROWS, D)

def backward_layer(layer_in, grad_top, route_rows, gain_vec, router_mat, w_gu, w_dn):
    blocks = ROWS // TOK_DEV
    h_wide, inv_rms, normed, expert_hits, slot_place, first_gate, second_gate, exp_rows, gate_part, up_part, sigmoid_gate, hidden = layer_state(layer_in, route_rows, gain_vec, router_mat, w_gu)
    grad_wide = grad_top.reshape(MICRO, blocks, TOK_DEV, D).astype(jnp.float32)
    gates = jnp.stack([first_gate, second_gate], axis=-1)
    scaled = rounded(gates[..., None] * grad_wide[..., None, :]).astype(jnp.float32)
    dy_rows = rounded(jnp.einsum('mbtkc,mbtkd->mbcd', slot_place, scaled, precision=lax.Precision.HIGHEST))
    dy_rows = dy_rows.astype(jnp.float32).reshape(MICRO, blocks, EXPERTS, CAP, D)
    d_hidden = jnp.einsum('mbecd,efd->mbecf', dy_rows, w_dn.astype(jnp.float32), precision=lax.Precision.HIGHEST)
    silu_gate = gate_part * sigmoid_gate
    silu_slope = sigmoid_gate * (1.0 + gate_part * (1.0 - sigmoid_gate))
    gate_up_grad = rounded(jnp.concatenate([d_hidden * up_part * silu_slope, d_hidden * silu_gate], axis=-1))
    gate_up_grad = gate_up_grad.astype(jnp.float32)
    rows_grad = rounded(jnp.einsum('mbecf,edf->mbecd', gate_up_grad, w_gu.astype(jnp.float32), precision=lax.Precision.HIGHEST))
    rows_grad = rows_grad.astype(jnp.float32).reshape(MICRO, blocks, EXPERTS * CAP, D)
    grad_gu = jnp.einsum('mbecd,mbecf->edf', exp_rows, gate_up_grad, precision=lax.Precision.HIGHEST)
    grad_dn = jnp.einsum('mbecf,mbecd->efd', hidden, dy_rows, precision=lax.Precision.HIGHEST)
    normed_grad = jnp.einsum('mbtkc,mbcd->mbtd', slot_place, rows_grad, precision=lax.Precision.HIGHEST)
    picked = jnp.einsum('mbtkc,mbcd->mbtkd', slot_place, expert_out(hidden, w_dn), precision=lax.Precision.HIGHEST)
    gate_grad = lax.optimization_barrier(jnp.sum(grad_wide[..., None, :] * picked, axis=-1))
    logit_grad = first_gate * second_gate * (gate_grad[..., 0] - gate_grad[..., 1])
    logit_cols = logit_grad[..., None] * (expert_hits[..., 0, :] - expert_hits[..., 1, :])
    normed_grad = normed_grad + jnp.einsum('mbte,de->mbtd', logit_cols, router_mat.astype(jnp.float32), precision=lax.Precision.HIGHEST)
    grad_rt = jnp.einsum('mbtd,mbte->de', normed, logit_cols, precision=lax.Precision.HIGHEST)
    grad_gn = lax.optimization_barrier(jnp.sum(normed_grad * h_wide * inv_rms, axis=(0, 1, 2)))
    scaled_grad = normed_grad * gain_vec
    projection = lax.optimization_barrier(jnp.mean(scaled_grad * h_wide, axis=-1, keepdims=True))
    input_grad = grad_wide + inv_rms * scaled_grad - h_wide * inv_rms * inv_rms * inv_rms * projection
    return (input_grad.astype(jnp.bfloat16).reshape(MICRO, ROWS, D), (grad_gu, grad_dn, grad_rt, grad_gn))

def reference(x_in, cotangent, route_ids, norm_gain, router, w_gate_up, w_down):

    def forward_step(layer_in, params):
        route_rows, gain_vec, router_mat, w_gu, w_dn = params
        return (forward_layer(layer_in, route_rows, gain_vec, router_mat, w_gu, w_dn), layer_in)
    _, inputs = lax.scan(forward_step, x_in, (route_ids, norm_gain, router, w_gate_up, w_down))

    def backward_step(grad_top, params):
        route_rows, gain_vec, router_mat, w_gu, w_dn, layer_in = params
        return backward_layer(layer_in, grad_top, route_rows, gain_vec, router_mat, w_gu, w_dn)
    grad_in, grad_list = lax.scan(backward_step, cotangent, (route_ids, norm_gain, router, w_gate_up, w_down, inputs), reverse=True)
    return (grad_in, grad_list[0], grad_list[1], grad_list[2], grad_list[3])
```

```python
import functools
import types

import jax
import jax.numpy as jnp
from jax import lax
from jax.experimental import pallas as pl
from jax.experimental.pallas import tpu as pltpu
from jax.sharding import PartitionSpec as P

EPS = 1e-05
CHUNKS = 8
LANES = 128
WEIGHT_STEPS = 4
LAG_F, LAG_T, LAG_B = (1, 2), (1, 2), (2, 4)
F32 = jnp.float32
BF16 = jnp.bfloat16
HIGH = lax.Precision.HIGHEST
ENDS, SEED, HX, GX, ROWS, GATE, BACK, TOP, DU, DOT, FIN = range(11)
KINDS = 11


def dot(a, b, dims, precision=None):
    return lax.dot_general(
        a, b, ((dims[:1], dims[1:]), ((), ())), precision=precision, preferred_element_type=F32
    )


def relay_body(cfg, names, *refs):
    r = types.SimpleNamespace(**dict(zip(names, refs)))
    chunks, n_rank, n_dp, n_sec, tok, cap = cfg
    _, tokens, piece = r.x.shape
    blk, width = r.u_land.shape[2:]
    cells = n_rank * blk
    hidden_width = r.w_dn.shape[0]
    n_expert = n_rank
    last = n_sec - 1
    section = lax.axis_index("section")
    me = lax.axis_index("expert") * n_dp + lax.axis_index("dp")
    send_sem, recv_sem = r.send_sem, r.recv_sem

    def place(step):
        rank = lax.rem(me + step, n_rank)
        return rank, {"expert": lax.div(rank, n_dp), "dp": lax.rem(rank, n_dp)}

    load_gu = pltpu.make_async_copy(r.w_gu, r.gu_buf, r.load_sem.at[0])
    load_dn = pltpu.make_async_copy(r.w_dn, r.dn_buf, r.load_sem.at[1])
    load_gu.start()
    load_dn.start()
    barrier = pltpu.get_barrier_semaphore()
    for step in range(1, n_sec):
        pl.semaphore_signal(
            barrier, inc=1, device_id={"section": lax.rem(section + step, n_sec)},
            device_id_type=pl.DeviceIdType.MESH,
        )
    for step in range(1, n_rank):
        pl.semaphore_signal(
            barrier, inc=1, device_id=place(step)[1], device_id_type=pl.DeviceIdType.MESH
        )
    r.rt[:n_expert] = r.router_t[...]
    r.rt[n_expert:] = r.router_t[...]
    r.acc[...] = jnp.zeros(r.acc.shape, F32)
    r.gain_acc[...] = jnp.zeros(r.gain_acc.shape, F32)

    def iota(shape, axis):
        return lax.broadcasted_iota(jnp.int32, shape, axis)

    def loop(count, body):
        def run(t, carry):
            body(t)
            return carry

        lax.fori_loop(0, count, run, 0)

    def tabulate(c):
        route = r.route[c].astype(F32)
        rows, cols = iota((tokens, tokens), 0), iota((tokens, tokens), 1)
        eye = (rows == cols).astype(F32)
        early = ((lax.div(rows, tok) == lax.div(cols, tok)) & (cols < rows)).astype(F32)
        across = [route[k : k + 1, :] for k in range(2)]
        e = [jnp.sum(eye * v, axis=1, keepdims=True) for v in across]
        within = (lax.div(iota((tokens, 1), 0), tok) * cap).astype(F32)
        inner, cell = [], []
        for k in range(2):
            named = (across[0] == e[k]).astype(F32) + (across[1] == e[k]).astype(F32)
            inner.append(within + jnp.sum(early * named, axis=1, keepdims=True))
            cell.append(e[k] * blk + inner[k])
            r.wide[c, k : k + 1] = across[k]
            r.wide[c, 2 + k : 3 + k] = jnp.sum(eye * cell[k], axis=0, keepdims=True)
        at = iota((tokens, LANES), 1)
        tall = jnp.zeros((tokens, LANES), F32)
        for k, v in enumerate(e + inner + cell):
            tall = jnp.where(at == k, v, tall)
        r.tall[c] = tall

    loop(chunks, tabulate)
    pl.semaphore_wait(barrier, n_rank - 1 + n_sec - 1)

    def push(src, dst, kind, c, device):
        pltpu.make_async_remote_copy(
            src_ref=src, dst_ref=dst, send_sem=send_sem.at[kind, c], recv_sem=recv_sem.at[kind, c],
            device_id=device, device_id_type=pl.DeviceIdType.MESH,
        ).start()

    def spread(src, dst, kind, c):
        for step in range(1, n_rank):
            rank, device = place(step)
            push(src.at[rank], dst.at[me], kind, c, device)
        dst[me] = src[me]

    def settle(ref, sem):
        pltpu.make_async_copy(ref, ref, sem).wait()

    def landed(dst, kind, c):
        settle(dst.at[pl.ds(0, n_rank - 1)], recv_sem.at[kind, c])

    def sent(src, kind, c):
        settle(src.at[pl.ds(0, n_rank - 1)], send_sem.at[kind, c])

    def lanes_of(value):
        return value.reshape(n_rank, 1, LANES)

    lane_of_cell = lax.rem(iota((cells, LANES), 0), blk) == iota((cells, LANES), 1)
    lane_of_cell = lane_of_cell.astype(F32)

    def columns(c):
        tall = r.tall[c]
        e, inner, cell = ([tall[:, 2 * i + k : 2 * i + k + 1] for k in range(2)] for i in range(3))
        return e, inner, cell

    def to_cells(c):
        at = iota((cells, tokens), 0).astype(F32)
        return [(r.wide[c, 2 + k : 3 + k] == at).astype(F32) for k in range(2)]

    def from_cells(cell):
        at = iota((tokens, cells), 1).astype(F32)
        return [(cell[k] == at).astype(F32) for k in range(2)]

    def hits(e):
        at = iota((tokens, n_expert), 1).astype(F32)
        return [(e[k] == at).astype(F32) for k in range(2)]

    def slots(inner):
        at = iota((tokens, LANES), 1).astype(F32)
        return [(inner[k] == at).astype(F32) for k in range(2)]

    def dispatch(place_at, value, out, land, kind, c):
        rows = dot(place_at.astype(BF16), value, (1, 0)).astype(BF16)
        out[...] = rows.reshape(n_rank, blk, width)
        spread(out, land, kind, c)

    def signed(e, l):
        l_high = l.astype(BF16).astype(F32)
        at = iota((tokens, 2 * n_expert), 1)
        which = lax.rem(at, n_expert).astype(F32)
        signs = (e[0] == which).astype(F32) - (e[1] == which).astype(F32)
        return (jnp.where(at < n_expert, l_high, l - l_high) * signs).astype(BF16)

    def add_router(c, cols):
        term = dot(cols, r.u[c], (0, 0))
        r.acc[...] += term[:n_expert] + term[n_expert:]

    def send_tokens(c):
        @pl.when(section == 0)
        def _():
            settle(r.ends.at[c, pl.ds(0, n_sec - 1)], recv_sem.at[ENDS, c])
            r.h[c] = jnp.concatenate(
                [r.x[c]] + [r.ends[c, s] for s in range(1, n_sec)], axis=1
            )

        @pl.when(section > 0)
        def _():
            settle(r.h.at[c], recv_sem.at[HX, c])

        place_at = to_cells(c)
        h = r.h[c].astype(F32)
        inv = lax.rsqrt(jnp.mean(h * h, axis=-1, keepdims=True) + EPS)
        u = (h * inv * r.gain[...]).astype(BF16)
        dispatch(place_at[0] + place_at[1], u, r.u_out.at[c], r.u_land.at[c], ROWS, c)
        r.u[c] = u
        e, inner, _ = columns(c)
        hit = hits(e)
        diff = jnp.sum((hit[0] - hit[1]) * dot(u, r.router_t[...], (1, 1)), axis=1, keepdims=True)
        gate = [jax.nn.sigmoid(diff), jax.nn.sigmoid(-diff)]
        at = iota((tokens, LANES), 1)
        r.keep[c] = jnp.where(at == 0, gate[0], jnp.where(at == 1, gate[1], inv))

        @pl.when(section == last)
        def _():
            slot = slots(inner)
            at = iota((n_expert, tokens), 0).astype(F32)
            packed = sum(
                dot((r.wide[c, k : k + 1] == at).astype(F32), gate[k] * slot[k], (1, 0), HIGH)
                for k in range(2)
            )
            r.gate_out[c] = lanes_of(packed)
            spread(r.gate_out.at[c], r.gate_land.at[c], GATE, c)

    def expert_up(c):
        @pl.when(c == 0)
        def _():
            load_gu.wait()
            load_dn.wait()

        landed(r.u_land.at[c], ROWS, c)
        rows = r.u_land[c].reshape(cells, width)
        r.rows[c] = rows
        gate_up = dot(rows, r.gu_buf[...], (1, 0))
        a, b = gate_up[:, :hidden_width], gate_up[:, hidden_width:]
        sig = jax.nn.sigmoid(a)
        silu = a * sig
        hidden = (silu * b).astype(BF16)
        r.hidden[c] = hidden
        r.slope[c, :, :hidden_width] = b * (sig * (1.0 + a * (1.0 - sig)))
        r.slope[c, :, hidden_width:] = silu
        return hidden

    def expert_forward(c):
        hidden = expert_up(c)
        y = dot(hidden, r.dn_buf[...], (1, 0)).astype(BF16)
        r.y_out[c] = y.reshape(n_rank, blk, width)
        spread(r.y_out.at[c], r.y_land.at[c], BACK, c)

    def expert_down(c, d_hidden):
        slope = r.slope[c]
        q = jnp.concatenate(
            [d_hidden * slope[:, :hidden_width], d_hidden * slope[:, hidden_width:]], axis=1
        ).astype(BF16)
        r.q[c] = q
        du = dot(q, r.gu_buf[...], (1, 1)).astype(BF16)
        r.du_out[c] = du.reshape(n_rank, blk, width)
        spread(r.du_out.at[c], r.du_land.at[c], DU, c)

    def expert_backward(c):
        landed(r.g_land.at[c], TOP, c)
        top = r.g_land[c].reshape(cells, width)
        r.dy[c] = top
        expert_down(c, dot(top, r.dn_buf[...], (1, 1)))

    def expert_last(c):
        hidden = expert_up(c)
        landed(r.g_land.at[c], TOP, c)
        landed(r.gate_land.at[c], GATE, c)
        spread_rows = (lax.div(iota((cells, n_rank), 0), blk) == iota((cells, n_rank), 1)).astype(F32)
        wide = dot(spread_rows, r.gate_land[c].reshape(n_rank, LANES), (1, 0), HIGH)
        gate = jnp.sum(wide * lane_of_cell, axis=1, keepdims=True)
        top = r.g_land[c].reshape(cells, width)
        plain = dot(top, r.dn_buf[...], (1, 1))
        expert_down(c, plain * gate)
        share = jnp.sum(plain * hidden.astype(F32), axis=1, keepdims=True)
        gather = (iota((n_rank, cells), 0) == lax.div(iota((n_rank, cells), 1), blk)).astype(F32)
        r.dot_out[c] = lanes_of(dot(gather, share * lane_of_cell, (1, 0), HIGH))
        spread(r.dot_out.at[c], r.dot_land.at[c], DOT, c)
        r.dy[c] = (top.astype(F32) * gate).astype(BF16)

    def combine_forward(c):
        pick = from_cells(columns(c)[2])
        keep = r.keep[c]
        landed(r.y_land.at[c], BACK, c)
        back = r.y_land[c].reshape(cells, width)
        picked = dot(jnp.concatenate(pick, axis=0).astype(BF16), back, (1, 0))
        h = r.h[c].astype(F32)
        up = h + keep[:, 0:1] * picked[:tokens] + keep[:, 1:2] * picked[tokens:]
        r.h_out[c] = up.astype(BF16)
        push(r.h_out.at[c], r.h.at[c], HX, c, {"section": section + 1})
        r.lean[c] = picked[:tokens] - picked[tokens:]

    def send_seed(c):
        settle(r.ends.at[c, pl.ds(0, n_sec - 1)], recv_sem.at[SEED, c])
        top = jnp.concatenate([r.ends[c, s] for s in range(last)] + [r.cot[c]], axis=1)
        r.g[c] = top
        place_at = to_cells(c)
        dispatch(place_at[0] + place_at[1], top, r.g_out.at[c], r.g_land.at[c], TOP, c)

    def send_top(c):
        place_at = jnp.concatenate(to_cells(c), axis=1)
        keep = r.keep[c]
        settle(r.g.at[c], recv_sem.at[GX, c])
        top = r.g[c].astype(F32)
        scaled = [(keep[:, k : k + 1] * top).astype(BF16) for k in range(2)]
        dispatch(
            place_at, jnp.concatenate(scaled, axis=0), r.g_out.at[c], r.g_land.at[c], TOP, c
        )
        share = jnp.sum(top * r.lean[c], axis=1, keepdims=True)
        cols = signed(columns(c)[0], keep[:, 0:1] * keep[:, 1:2] * share)
        r.cols[c] = cols
        add_router(c, cols)

        @pl.when(c == chunks - 1)
        def _():
            router_start()

    def finish_last(c):
        e, inner, cell = columns(c)
        hit, slot = hits(e), slots(inner)
        keep = r.keep[c]
        landed(r.dot_land.at[c], DOT, c)
        shares = r.dot_land[c].reshape(n_rank, LANES)
        wide = [dot(hit[k], shares, (1, 0), HIGH) * slot[k] for k in range(2)]
        share = jnp.sum(wide[0] - wide[1], axis=1, keepdims=True)
        cols = signed(e, keep[:, 0:1] * keep[:, 1:2] * share)
        finish(c, cols)
        add_router(c, cols)

    def finish(c, cols):
        pick = from_cells(columns(c)[2])
        inv = r.keep[c][:, 2:3]
        extra = dot(cols, r.rt[...], (1, 0))
        hn = r.h[c].astype(F32) * inv
        landed(r.du_land.at[c], DU, c)
        back = r.du_land[c].reshape(cells, width)
        du = dot((pick[0] + pick[1]).astype(BF16), back, (1, 0)) + extra
        scaled = du * r.gain[...]
        projection = jnp.mean(scaled * hn, axis=-1, keepdims=True)
        low = (r.g[c].astype(F32) + inv * (scaled - hn * projection)).astype(BF16)
        r.low[c] = low

        @pl.when(section > 0)
        def _():
            push(r.low.at[c], r.g.at[c], GX, c, {"section": section - 1})

        @pl.when(section == 0)
        def _():
            r.gin[c] = low[:, :piece]
            for s in range(1, n_sec):
                r.fin[c, s - 1] = low[:, s * piece : (s + 1) * piece]
                push(r.fin.at[c, s - 1], r.gin.at[c], FIN, c, {"section": s})

        r.gain_acc[...] += jnp.sum(du * hn, axis=0, keepdims=True)

    part = width // n_rank

    def share_out(src, dst, which):
        for step in range(1, n_rank):
            rank, device = place(step)
            pltpu.make_async_remote_copy(
                src_ref=src(rank), dst_ref=dst.at[me],
                send_sem=r.sum_sem.at[2 * which], recv_sem=r.sum_sem.at[2 * which + 1],
                device_id=device, device_id_type=pl.DeviceIdType.MESH,
            ).start()
        dst[me] = src(me)[...]

    def shared(dst, which, side):
        settle(dst.at[pl.ds(0, n_rank - 1)], r.sum_sem.at[2 * which + side])

    def router_start():
        for rank in range(n_rank):
            r.part_out[rank] = r.acc[:, rank * part : (rank + 1) * part].astype(BF16)
        share_out(lambda rank: r.part_out.at[rank], r.part_land, 0)

    def router_middle():
        shared(r.part_land, 0, 1)
        r.tot_out[...] = jnp.sum(r.part_land[...].astype(F32), axis=0).astype(BF16)
        share_out(lambda rank: r.tot_out, r.tot_land, 1)

    for c in range(chunks):
        @pl.when(section > 0)
        def _():
            push(r.x.at[c], r.ends.at[c, section], ENDS, c, {"section": 0})

        @pl.when(section < last)
        def _():
            push(r.cot.at[c], r.ends.at[c, section], SEED, c, {"section": last})

    def guarded(t, body):
        @pl.when((t >= 0) & (t < chunks))
        def _():
            body(jnp.clip(t, 0, chunks - 1))

    def rounds(stages):
        def step(t):
            for lag, body in stages:
                guarded(t - lag, body)

        loop(chunks + max(lag for lag, _ in stages), step)

    @pl.when(section == last)
    def _():
        loop(chunks, send_seed)
        rounds(((0, send_tokens), (LAG_T[0], expert_last), (LAG_T[1], finish_last)))
        router_start()
        router_middle()

    @pl.when(section < last)
    def _():
        rounds(((0, send_tokens), (LAG_F[0], expert_forward), (LAG_F[1], combine_forward)))

        def middle(c):
            @pl.when(c == chunks - 1)
            def _():
                router_middle()

        rounds((
            (0, send_top), (LAG_B[0], expert_backward), (LAG_B[0], middle),
            (LAG_B[1], lambda c: finish(c, r.cols[c])),
        ))

    lines = width // LANES
    r.gain_out[...] = jnp.concatenate(
        [r.gain_acc[:, i * LANES : (i + 1) * LANES] for i in range(lines)], axis=0
    ).astype(BF16)
    share_out(lambda rank: r.gain_out, r.gain_land, 2)
    shared(r.tot_land, 1, 1)
    for rank in range(n_rank):
        r.grad_router[:, rank * part : (rank + 1) * part] = r.tot_land[rank].astype(F32)
    shared(r.gain_land, 2, 1)
    total = jnp.sum(r.gain_land[...].astype(F32), axis=0)
    for i in range(lines):
        r.grad_gain[:, i * LANES : (i + 1) * LANES] = total[i : i + 1]
    shared(r.part_land, 0, 0)
    shared(r.tot_land, 1, 0)
    shared(r.gain_land, 2, 0)

    for c in range(chunks):
        for kind, ref in ((ROWS, r.u_out), (TOP, r.g_out), (DU, r.du_out)):
            sent(ref.at[c], kind, c)

        @pl.when(section == last)
        def _():
            sent(r.gate_out.at[c], GATE, c)
            sent(r.dot_out.at[c], DOT, c)

        @pl.when(section < last)
        def _():
            sent(r.y_out.at[c], BACK, c)
            settle(r.h_out.at[c], send_sem.at[HX, c])
            settle(r.cot.at[c], send_sem.at[SEED, c])

        @pl.when(section == 0)
        def _():
            settle(r.fin.at[c], send_sem.at[FIN, c])

        @pl.when(section > 0)
        def _():
            settle(r.x.at[c], send_sem.at[ENDS, c])
            settle(r.low.at[c], send_sem.at[GX, c])
            settle(r.gin.at[c], recv_sem.at[FIN, c])


def weight_body(rows, q, hidden, dy, *refs):
    grad_gu, grad_dn = refs[len(refs) // 2 - 1 : len(refs) // 2 + 1]
    grad_gu[...] = dot(rows[...], q[...], (0, 0))
    grad_dn[...] = dot(hidden[...], dy[...], (0, 0))

    @pl.when(pl.program_id(0) == 0)
    def _():
        count = (len(refs) - 2) // 2
        for given, kept in zip(refs[:count], refs[count + 2 :]):
            kept[...] = given[...]


def weight_grads(rows, q, hidden, dy, *others):
    count, width = rows.shape
    hidden_width = hidden.shape[1]
    steps = WEIGHT_STEPS

    def whole(a):
        return pl.BlockSpec(a.shape, lambda i: (0,) * a.ndim)

    return pl.pallas_call(
        weight_body,
        grid=(steps,),
        out_shape=[
            jax.ShapeDtypeStruct((width, 2 * hidden_width), F32),
            jax.ShapeDtypeStruct((hidden_width, width), F32),
        ]
        + [jax.ShapeDtypeStruct(a.shape, a.dtype) for a in others],
        in_specs=[
            pl.BlockSpec((count, width // steps), lambda i: (0, i)),
            pl.BlockSpec((count, 2 * hidden_width), lambda i: (0, 0)),
            pl.BlockSpec((count, hidden_width // steps), lambda i: (0, i)),
            pl.BlockSpec((count, width), lambda i: (0, 0)),
        ]
        + [whole(a) for a in others],
        out_specs=[
            pl.BlockSpec((width // steps, 2 * hidden_width), lambda i: (i, 0)),
            pl.BlockSpec((hidden_width // steps, width), lambda i: (i, 0)),
        ]
        + [whole(a) for a in others],
        compiler_params=pltpu.CompilerParams(vmem_limit_bytes=60 * 1024 * 1024),
    )(rows, q, hidden, dy, *others)


def local(x_in, cotangent, route_ids, norm_gain, router, w_gate_up, w_down):
    micro, tok, piece = x_in.shape
    n_sec = lax.axis_size("section")
    n_dp = lax.axis_size("dp")
    n_rank = lax.axis_size("expert") * n_dp
    per_rank, hidden_width, width = w_down.shape[1:]
    assert per_rank == 1 and n_sec > 1
    cap = tok * 2 * 9 // (8 * n_rank)
    chunks = CHUNKS if micro % CHUNKS == 0 else 1
    per = micro // chunks
    tokens, blk = per * tok, per * cap
    cells = n_rank * blk
    part = width // n_rank
    args = dict(
        x=x_in.reshape(chunks, tokens, piece), cot=cotangent.reshape(chunks, tokens, piece),
        route=jnp.transpose(route_ids.reshape(chunks, tokens, 2), (0, 2, 1)),
        gain=norm_gain, router_t=router[0].T,
        w_gu=w_gate_up[0, 0], w_dn=w_down[0, 0],
    )
    outs = dict(
        rows=((chunks, cells, width), BF16), q=((chunks, cells, 2 * hidden_width), BF16),
        hidden=((chunks, cells, hidden_width), BF16), dy=((chunks, cells, width), BF16),
        gin=((chunks, tokens, piece), BF16), grad_router=((n_rank, width), F32),
        grad_gain=((1, width), F32),
    )
    exchanged = ((chunks, n_rank, blk, width), BF16)
    token_rows = ((chunks, tokens, width), BF16)
    line = ((chunks, n_rank, 1, LANES), F32)
    scratch = dict(
        gu_buf=(w_gate_up[0, 0].shape, BF16), dn_buf=(w_down[0, 0].shape, BF16),
        rt=((2 * n_rank, width), BF16), acc=((n_rank, width), F32), gain_acc=((1, width), F32),
        tall=((chunks, tokens, LANES), F32), wide=((chunks, 8, tokens), F32),
        lean=((chunks, tokens, width), F32), cols=((chunks, tokens, 2 * n_rank), BF16),
        gain_out=((width // LANES, LANES), BF16), gain_land=((n_rank, width // LANES, LANES), BF16),
        ends=((chunks, n_sec, tokens, piece), BF16), fin=((chunks, n_sec - 1, tokens, piece), BF16),
        h=token_rows, u=token_rows, g=token_rows, h_out=token_rows, low=token_rows,
        keep=((chunks, tokens, LANES), F32), slope=((chunks, cells, 2 * hidden_width), F32),
        part_out=((n_rank, n_rank, part), BF16), part_land=((n_rank, n_rank, part), BF16),
        tot_out=((n_rank, part), BF16), tot_land=((n_rank, n_rank, part), BF16),
        u_out=exchanged, u_land=exchanged, y_out=exchanged, y_land=exchanged,
        g_out=exchanged, g_land=exchanged, du_out=exchanged, du_land=exchanged,
        gate_out=line, gate_land=line, dot_out=line, dot_land=line,
    )
    sems = dict(load_sem=(2,), send_sem=(KINDS, chunks), recv_sem=(KINDS, chunks), sum_sem=(6,))
    vmem = pl.BlockSpec(memory_space=pltpu.VMEM)
    hbm = pl.BlockSpec(memory_space=pl.ANY)
    cfg = (chunks, n_rank, n_dp, n_sec, tok, cap)
    made = pl.pallas_call(
        functools.partial(relay_body, cfg, list(args) + list(outs) + list(scratch) + list(sems)),
        out_shape=[jax.ShapeDtypeStruct(*v) for v in outs.values()],
        in_specs=[hbm if k in ("w_gu", "w_dn") else vmem for k in args],
        out_specs=[vmem] * len(outs),
        scratch_shapes=[pltpu.VMEM(*v) for v in scratch.values()]
        + [pltpu.SemaphoreType.DMA(v) for v in sems.values()],
        compiler_params=pltpu.CompilerParams(
            collective_id=1, has_side_effects=True, vmem_limit_bytes=56 * 1024 * 1024
        ),
    )(*args.values())
    made = types.SimpleNamespace(**dict(zip(outs, made)))

    def flat(value):
        return value.reshape(chunks * cells, -1)

    grad_gu, grad_dn, gin, grad_router, grad_gain = weight_grads(
        flat(made.rows), flat(made.q), flat(made.hidden), flat(made.dy),
        made.gin, made.grad_router, made.grad_gain,
    )
    return (
        gin.reshape(micro, tok, piece), grad_gu[None, None], grad_dn[None, None],
        grad_router.T[None], grad_gain,
    )


def solution(mesh):
    in_specs = (
        P(None, ("expert", "dp"), "section"),
        P(None, ("expert", "dp"), "section"),
        P("section", None, ("expert", "dp"), None),
        P("section", None),
        P("section", None, None),
        P("section", ("expert", "dp"), None, None),
        P("section", ("expert", "dp"), None, None),
    )
    out_specs = (
        P(None, ("expert", "dp"), "section"),
        P("section", ("expert", "dp"), None, None),
        P("section", ("expert", "dp"), None, None),
        P("section", None, None),
        P("section", None),
    )
    return jax.shard_map(local, mesh=mesh, in_specs=in_specs, out_specs=out_specs, check_vma=False)
```

```python
import functools
import types

import jax
import jax.numpy as jnp
from jax import lax
from jax.experimental import pallas as pl
from jax.experimental.pallas import tpu as pltpu
from jax.sharding import PartitionSpec as P

EPS = 1e-05
CHUNKS = 8
LANES = 128
WEIGHT_STEPS = 4
LIMIT_RELAY = 56
LIMIT_WEIGHT = 48
LAG_S = 5
LAG_F, LAG_T, LAG_B = (2, 3), (1, 2), (2, 4)
F32 = jnp.float32
BF16 = jnp.bfloat16
HIGH = lax.Precision.HIGHEST
ENDS, SEED, HX, GX, ROWS, GATE, BACK, TOP, DU, DOT, FIN = range(11)
KINDS = 11


def dot(a, b, dims, precision=None):
    return lax.dot_general(
        a, b, ((dims[:1], dims[1:]), ((), ())), precision=precision, preferred_element_type=F32
    )


def relay_body(cfg, names, *refs):
    r = types.SimpleNamespace(**dict(zip(names, refs)))
    chunks, n_rank, n_dp, n_sec, tok, cap = cfg
    _, tokens, piece = r.x.shape
    blk, width = r.u_land.shape[2:]
    cells = n_rank * blk
    hidden_width = r.w_dn.shape[0]
    n_expert = n_rank
    last = n_sec - 1
    section = lax.axis_index("section")
    me = lax.axis_index("expert") * n_dp + lax.axis_index("dp")
    send_sem, recv_sem = r.send_sem, r.recv_sem

    def place(step):
        rank = lax.rem(me + step, n_rank)
        return rank, {"expert": lax.div(rank, n_dp), "dp": lax.rem(rank, n_dp)}

    load_gu = pltpu.make_async_copy(r.w_gu, r.gu_buf, r.load_sem.at[0])
    load_dn = pltpu.make_async_copy(r.w_dn, r.dn_buf, r.load_sem.at[1])
    loads = [
        pltpu.make_async_copy(src, dst, r.load_sem.at[2 + i])
        for i, (src, dst) in enumerate((
            (r.x_hbm, r.x), (r.cot_hbm, r.cot), (r.route_hbm, r.route), (r.gain_hbm, r.gain),
            (r.router_hbm, r.router_t),
        ))
    ]
    for load in loads:
        load.start()
    load_gu.start()
    load_dn.start()
    barrier = pltpu.get_barrier_semaphore()
    for step in range(1, n_sec):
        pl.semaphore_signal(
            barrier, inc=1, device_id={"section": lax.rem(section + step, n_sec)},
            device_id_type=pl.DeviceIdType.MESH,
        )
    for step in range(1, n_rank):
        pl.semaphore_signal(
            barrier, inc=1, device_id=place(step)[1], device_id_type=pl.DeviceIdType.MESH
        )
    def iota(shape, axis):
        return lax.broadcasted_iota(jnp.int32, shape, axis)

    def loop(count, body):
        def run(t, carry):
            body(t)
            return carry

        lax.fori_loop(0, count, run, 0)

    def tabulate(c):
        route = r.route[c].astype(F32)
        rows, cols = iota((tokens, tokens), 0), iota((tokens, tokens), 1)
        eye = (rows == cols).astype(F32)
        early = ((lax.div(rows, tok) == lax.div(cols, tok)) & (cols < rows)).astype(F32)
        across = [route[k : k + 1, :] for k in range(2)]
        e = [jnp.sum(eye * v, axis=1, keepdims=True) for v in across]
        within = (lax.div(iota((tokens, 1), 0), tok) * cap).astype(F32)
        inner, cell = [], []
        for k in range(2):
            named = (across[0] == e[k]).astype(F32) + (across[1] == e[k]).astype(F32)
            inner.append(within + jnp.sum(early * named, axis=1, keepdims=True))
            cell.append(e[k] * blk + inner[k])
            r.wide[c, k : k + 1] = across[k]
            r.wide[c, 2 + k : 3 + k] = jnp.sum(eye * cell[k], axis=0, keepdims=True)
        at = iota((tokens, LANES), 1)
        tall = jnp.zeros((tokens, LANES), F32)
        for k, v in enumerate(e + inner + cell):
            tall = jnp.where(at == k, v, tall)
        r.tall[c] = tall

    pl.semaphore_wait(barrier, n_rank - 1 + n_sec - 1)
    for load in loads:
        load.wait()

    def push(src, dst, kind, c, device):
        pltpu.make_async_remote_copy(
            src_ref=src, dst_ref=dst, send_sem=send_sem.at[kind, c], recv_sem=recv_sem.at[kind, c],
            device_id=device, device_id_type=pl.DeviceIdType.MESH,
        ).start()

    for c in range(chunks):
        @pl.when(section > 0)
        def _():
            push(r.x.at[c], r.ends.at[c, section], ENDS, c, {"section": 0})

        @pl.when(section < last)
        def _():
            push(r.cot.at[c], r.ends.at[c, section], SEED, c, {"section": last})

    r.rt[:n_expert] = r.router_t[...]
    r.rt[n_expert:] = r.router_t[...]
    r.acc[...] = jnp.zeros(r.acc.shape, F32)
    r.gain_acc[...] = jnp.zeros(r.gain_acc.shape, F32)

    for c in range(chunks):
        tabulate(c)

    def spread(src, dst, kind, c):
        for step in range(1, n_rank):
            rank, device = place(step)
            push(src.at[rank], dst.at[me], kind, c, device)
        dst[me] = src[me]

    def settle(ref, sem):
        pltpu.make_async_copy(ref, ref, sem).wait()

    def landed(dst, kind, c):
        settle(dst.at[pl.ds(0, n_rank - 1)], recv_sem.at[kind, c])

    def sent(src, kind, c):
        settle(src.at[pl.ds(0, n_rank - 1)], send_sem.at[kind, c])

    def lanes_of(value):
        return value.reshape(n_rank, 1, LANES)

    lane_of_cell = lax.rem(iota((cells, LANES), 0), blk) == iota((cells, LANES), 1)
    lane_of_cell = lane_of_cell.astype(F32)

    def columns(c):
        tall = r.tall[c]
        e, inner, cell = ([tall[:, 2 * i + k : 2 * i + k + 1] for k in range(2)] for i in range(3))
        return e, inner, cell

    def to_cells(c):
        at = iota((cells, tokens), 0).astype(F32)
        return [(r.wide[c, 2 + k : 3 + k] == at).astype(F32) for k in range(2)]

    def from_cells(cell):
        at = iota((tokens, cells), 1).astype(F32)
        return [(cell[k] == at).astype(F32) for k in range(2)]

    def hits(e):
        at = iota((tokens, n_expert), 1).astype(F32)
        return [(e[k] == at).astype(F32) for k in range(2)]

    def slots(inner):
        at = iota((tokens, LANES), 1).astype(F32)
        return [(inner[k] == at).astype(F32) for k in range(2)]

    def dispatch(place_at, value, out, land, kind, c):
        rows = dot(place_at.astype(BF16), value, (1, 0)).astype(BF16)
        out[...] = rows.reshape(n_rank, blk, width)
        spread(out, land, kind, c)

    def signed(e, l):
        l_high = l.astype(BF16).astype(F32)
        at = iota((tokens, 2 * n_expert), 1)
        which = lax.rem(at, n_expert).astype(F32)
        signs = (e[0] == which).astype(F32) - (e[1] == which).astype(F32)
        return (jnp.where(at < n_expert, l_high, l - l_high) * signs).astype(BF16)

    def add_router(c, cols):
        term = dot(cols, r.u[c], (0, 0))
        r.acc[...] += term[:n_expert] + term[n_expert:]

    def send_tokens(c):
        @pl.when(section == 0)
        def _():
            settle(r.ends.at[c, pl.ds(0, n_sec - 1)], recv_sem.at[ENDS, c])
            r.h[c] = jnp.concatenate(
                [r.x[c]] + [r.ends[c, s] for s in range(1, n_sec)], axis=1
            )

        @pl.when(section > 0)
        def _():
            settle(r.h.at[c], recv_sem.at[HX, c])

        place_at = to_cells(c)
        h = r.h[c].astype(F32)
        inv = lax.rsqrt(jnp.mean(h * h, axis=-1, keepdims=True) + EPS)
        u = (h * inv * r.gain[...]).astype(BF16)
        dispatch(place_at[0] + place_at[1], u, r.u_out.at[c], r.u_land.at[c], ROWS, c)
        r.u[c] = u
        e, inner, _ = columns(c)
        hit = hits(e)
        diff = jnp.sum((hit[0] - hit[1]) * dot(u, r.router_t[...], (1, 1)), axis=1, keepdims=True)
        gate = [jax.nn.sigmoid(diff), jax.nn.sigmoid(-diff)]
        at = iota((tokens, LANES), 1)
        r.keep[c] = jnp.where(at == 0, gate[0], jnp.where(at == 1, gate[1], inv))

        @pl.when(section == last)
        def _():
            slot = slots(inner)
            at = iota((n_expert, tokens), 0).astype(F32)
            packed = sum(
                dot((r.wide[c, k : k + 1] == at).astype(F32), gate[k] * slot[k], (1, 0), HIGH)
                for k in range(2)
            )
            r.gate_out[c] = lanes_of(packed)
            spread(r.gate_out.at[c], r.gate_land.at[c], GATE, c)

    def expert_up(c):
        @pl.when(c == 0)
        def _():
            load_gu.wait()

        landed(r.u_land.at[c], ROWS, c)
        rows = r.u_land[c].reshape(cells, width)
        r.rows[c] = rows
        gate_up = dot(rows, r.gu_buf[...], (1, 0))
        a, b = gate_up[:, :hidden_width], gate_up[:, hidden_width:]
        sig = jax.nn.sigmoid(a)
        silu = a * sig
        hidden = (silu * b).astype(BF16)
        r.hidden[c] = hidden
        r.slope[c, :, :hidden_width] = b * (sig * (1.0 + a * (1.0 - sig)))
        r.slope[c, :, hidden_width:] = silu
        return hidden

    def expert_forward(c):
        hidden = expert_up(c)

        @pl.when(c == 0)
        def _():
            load_dn.wait()

        y = dot(hidden, r.dn_buf[...], (1, 0)).astype(BF16)
        r.y_out[c] = y.reshape(n_rank, blk, width)
        spread(r.y_out.at[c], r.y_land.at[c], BACK, c)

    def expert_down(c, d_hidden):
        slope = r.slope[c]
        q = jnp.concatenate(
            [d_hidden * slope[:, :hidden_width], d_hidden * slope[:, hidden_width:]], axis=1
        ).astype(BF16)
        r.q[c] = q
        du = dot(q, r.gu_buf[...], (1, 1)).astype(BF16)
        r.du_out[c] = du.reshape(n_rank, blk, width)
        spread(r.du_out.at[c], r.du_land.at[c], DU, c)
        both = r.rows[c].astype(F32) * du.astype(F32)
        r.gain_acc[...] += jnp.sum(both, axis=0, keepdims=True)

        @pl.when(c == chunks - 1)
        def _():
            r.gain_out[...] = jnp.concatenate(
                [r.gain_acc[:, i * LANES : (i + 1) * LANES] for i in range(lines)], axis=0
            ).astype(BF16)
            share_out(lambda rank: r.gain_out, r.gain_land, 2)

    def expert_backward(c):
        landed(r.g_land.at[c], TOP, c)
        top = r.g_land[c].reshape(cells, width)
        r.dy[c] = top
        expert_down(c, dot(top, r.dn_buf[...], (1, 1)))

    def expert_last(c):
        hidden = expert_up(c)
        landed(r.gate_land.at[c], GATE, c)
        spread_rows = (lax.div(iota((cells, n_rank), 0), blk) == iota((cells, n_rank), 1)).astype(F32)
        wide = dot(spread_rows, r.gate_land[c].reshape(n_rank, LANES), (1, 0), HIGH)
        gate = jnp.sum(wide * lane_of_cell, axis=1, keepdims=True)
        top = r.g_land[c].reshape(cells, width)
        plain = r.plain[c]
        expert_down(c, plain * gate)
        share = jnp.sum(plain * hidden.astype(F32), axis=1, keepdims=True)
        gather = (iota((n_rank, cells), 0) == lax.div(iota((n_rank, cells), 1), blk)).astype(F32)
        r.dot_out[c] = lanes_of(dot(gather, share * lane_of_cell, (1, 0), HIGH))
        spread(r.dot_out.at[c], r.dot_land.at[c], DOT, c)
        r.dy[c] = (top.astype(F32) * gate).astype(BF16)

    def combine_forward(c):
        pick = from_cells(columns(c)[2])
        keep = r.keep[c]
        landed(r.y_land.at[c], BACK, c)
        back = r.y_land[c].reshape(cells, width)
        picked = dot(jnp.concatenate(pick, axis=0).astype(BF16), back, (1, 0))
        h = r.h[c].astype(F32)
        up = h + keep[:, 0:1] * picked[:tokens] + keep[:, 1:2] * picked[tokens:]
        r.h_out[c] = up.astype(BF16)
        push(r.h_out.at[c], r.h.at[c], HX, c, {"section": section + 1})
        r.lean[c] = picked[:tokens] - picked[tokens:]

    def send_seed(c):
        settle(r.ends.at[c, pl.ds(0, n_sec - 1)], recv_sem.at[SEED, c])
        top = jnp.concatenate([r.ends[c, s] for s in range(last)] + [r.cot[c]], axis=1)
        r.g[c] = top
        place_at = to_cells(c)
        dispatch(place_at[0] + place_at[1], top, r.g_out.at[c], r.g_land.at[c], TOP, c)

    def expert_seed(c):
        @pl.when(c == 0)
        def _():
            load_dn.wait()

        landed(r.g_land.at[c], TOP, c)
        r.plain[c] = dot(r.g_land[c].reshape(cells, width), r.dn_buf[...], (1, 1))

    def send_top(c):
        place_at = jnp.concatenate(to_cells(c), axis=1)
        keep = r.keep[c]
        settle(r.g.at[c], recv_sem.at[GX, c])
        top = r.g[c].astype(F32)
        scaled = [(keep[:, k : k + 1] * top).astype(BF16) for k in range(2)]
        dispatch(
            place_at, jnp.concatenate(scaled, axis=0), r.g_out.at[c], r.g_land.at[c], TOP, c
        )
        share = jnp.sum(top * r.lean[c], axis=1, keepdims=True)
        cols = signed(columns(c)[0], keep[:, 0:1] * keep[:, 1:2] * share)
        r.cols[c] = cols
        add_router(c, cols)

        @pl.when(c == chunks - 1)
        def _():
            router_start()

    def finish_last(c):
        e, inner, cell = columns(c)
        hit, slot = hits(e), slots(inner)
        keep = r.keep[c]
        landed(r.dot_land.at[c], DOT, c)
        shares = r.dot_land[c].reshape(n_rank, LANES)
        wide = [dot(hit[k], shares, (1, 0), HIGH) * slot[k] for k in range(2)]
        share = jnp.sum(wide[0] - wide[1], axis=1, keepdims=True)
        cols = signed(e, keep[:, 0:1] * keep[:, 1:2] * share)
        finish(c, cols)
        add_router(c, cols)

    def finish(c, cols):
        pick = from_cells(columns(c)[2])
        inv = r.keep[c][:, 2:3]
        extra = dot(cols, r.rt[...], (1, 0))
        hn = r.h[c].astype(F32) * inv
        landed(r.du_land.at[c], DU, c)
        back = r.du_land[c].reshape(cells, width)
        du = dot((pick[0] + pick[1]).astype(BF16), back, (1, 0)) + extra
        scaled = du * r.gain[...]
        projection = jnp.mean(scaled * hn, axis=-1, keepdims=True)
        low = (r.g[c].astype(F32) + inv * (scaled - hn * projection)).astype(BF16)
        r.low[c] = low

        @pl.when(section > 0)
        def _():
            push(r.low.at[c], r.g.at[c], GX, c, {"section": section - 1})

        @pl.when(section == 0)
        def _():
            r.gin[c] = low[:, :piece]
            for s in range(1, n_sec):
                r.fin[c, s - 1] = low[:, s * piece : (s + 1) * piece]
                push(r.fin.at[c, s - 1], r.gin.at[c], FIN, c, {"section": s})

    part, lines = width // n_rank, width // LANES

    def share_out(src, dst, which):
        for step in range(1, n_rank):
            rank, device = place(step)
            pltpu.make_async_remote_copy(
                src_ref=src(rank), dst_ref=dst.at[me],
                send_sem=r.sum_sem.at[2 * which], recv_sem=r.sum_sem.at[2 * which + 1],
                device_id=device, device_id_type=pl.DeviceIdType.MESH,
            ).start()
        dst[me] = src(me)[...]

    def shared(dst, which, side):
        settle(dst.at[pl.ds(0, n_rank - 1)], r.sum_sem.at[2 * which + side])

    def router_start():
        for rank in range(n_rank):
            r.part_out[rank] = r.acc[:, rank * part : (rank + 1) * part].astype(BF16)
        share_out(lambda rank: r.part_out.at[rank], r.part_land, 0)

    def router_middle():
        shared(r.part_land, 0, 1)
        r.tot_out[...] = jnp.sum(r.part_land[...].astype(F32), axis=0).astype(BF16)
        share_out(lambda rank: r.tot_out, r.tot_land, 1)

    def guarded(t, body):
        @pl.when((t >= 0) & (t < chunks))
        def _():
            body(jnp.clip(t, 0, chunks - 1))

    def rounds(stages):
        def step(t):
            for lag, body in stages:
                guarded(t - lag, body)

        loop(chunks + max(lag for lag, _ in stages), step)

    @pl.when(section == last)
    def _():
        rounds(((0, send_seed), (LAG_S, expert_seed)))
        rounds(((0, send_tokens), (LAG_T[0], expert_last), (LAG_T[1], finish_last)))
        router_start()
        router_middle()

    @pl.when(section < last)
    def _():
        rounds(((0, send_tokens), (LAG_F[0], expert_forward), (LAG_F[1], combine_forward)))

        def middle(c):
            @pl.when(c == chunks - 1)
            def _():
                router_middle()

        rounds((
            (0, send_top), (LAG_B[0], expert_backward), (LAG_B[0], middle),
            (LAG_B[1], lambda c: finish(c, r.cols[c])),
        ))

    shared(r.tot_land, 1, 1)
    for rank in range(n_rank):
        r.grad_router[:, rank * part : (rank + 1) * part] = r.tot_land[rank].astype(F32)
    shared(r.gain_land, 2, 1)
    total = jnp.sum(r.gain_land[...].astype(F32), axis=0)
    routed = jnp.sum(r.router_t[...].astype(F32) * r.grad_router[...], axis=0, keepdims=True)
    for i in range(lines):
        lane = slice(i * LANES, (i + 1) * LANES)
        r.grad_gain[:, lane] = (total[i : i + 1] + routed[:, lane]) / r.gain[:, lane]
    shared(r.part_land, 0, 0)
    shared(r.tot_land, 1, 0)
    shared(r.gain_land, 2, 0)

    for c in range(chunks):
        for kind, ref in ((ROWS, r.u_out), (TOP, r.g_out), (DU, r.du_out)):
            sent(ref.at[c], kind, c)

        @pl.when(section == last)
        def _():
            sent(r.gate_out.at[c], GATE, c)
            sent(r.dot_out.at[c], DOT, c)

        @pl.when(section < last)
        def _():
            sent(r.y_out.at[c], BACK, c)
            settle(r.h_out.at[c], send_sem.at[HX, c])
            settle(r.cot.at[c], send_sem.at[SEED, c])

        @pl.when(section == 0)
        def _():
            settle(r.fin.at[c], send_sem.at[FIN, c])

        @pl.when(section > 0)
        def _():
            settle(r.x.at[c], send_sem.at[ENDS, c])
            settle(r.low.at[c], send_sem.at[GX, c])
            settle(r.gin.at[c], recv_sem.at[FIN, c])


def weight_body(steps, n_other, *refs):
    rows, q, hidden, dy = refs[:4]
    others = refs[4 : 4 + n_other]
    grad_gu, grad_dn = refs[4 + n_other : 6 + n_other]
    kept = refs[6 + n_other : 6 + 2 * n_other]
    up, down, sem = refs[6 + 2 * n_other :]
    for given, copy in zip(others, kept):
        copy[...] = given[...]
    writes = []
    for i in range(steps):
        for k, (buf, out, left, right) in enumerate(
            ((up, grad_gu, rows, q), (down, grad_dn, hidden, dy))
        ):
            size = buf.shape[0] // steps
            at = pl.ds(i * size, size)
            buf[at] = dot(left[:, at], right[...], (0, 0))
            write = pltpu.make_async_copy(buf.at[at], out.at[at], sem.at[k, i])
            write.start()
            writes.append(write)
    for write in writes:
        write.wait()


def weight_grads(rows, q, hidden, dy, *others):
    width, hidden_width = rows.shape[1], hidden.shape[1]
    shapes = [(width, 2 * hidden_width), (hidden_width, width)]
    vmem, hbm = pl.BlockSpec(memory_space=pltpu.VMEM), pl.BlockSpec(memory_space=pltpu.HBM)
    return pl.pallas_call(
        functools.partial(weight_body, WEIGHT_STEPS, len(others)),
        out_shape=[jax.ShapeDtypeStruct(v, F32) for v in shapes]
        + [jax.ShapeDtypeStruct(a.shape, a.dtype) for a in others],
        in_specs=[vmem] * (4 + len(others)),
        out_specs=[hbm] * 2 + [vmem] * len(others),
        scratch_shapes=[pltpu.VMEM(v, F32) for v in shapes]
        + [pltpu.SemaphoreType.DMA((2, WEIGHT_STEPS))],
        compiler_params=pltpu.CompilerParams(vmem_limit_bytes=LIMIT_WEIGHT * 1024 * 1024),
    )(rows, q, hidden, dy, *others)


def local(x_in, cotangent, route_ids, norm_gain, router, w_gate_up, w_down):
    micro, tok, piece = x_in.shape
    n_sec = lax.axis_size("section")
    n_dp = lax.axis_size("dp")
    n_rank = lax.axis_size("expert") * n_dp
    per_rank, hidden_width, width = w_down.shape[1:]
    assert per_rank == 1 and n_sec > 1
    cap = tok * 2 * 9 // (8 * n_rank)
    chunks = CHUNKS if micro % CHUNKS == 0 else 1
    per = micro // chunks
    tokens, blk = per * tok, per * cap
    cells = n_rank * blk
    part = width // n_rank
    args = dict(
        x_hbm=x_in.reshape(chunks, tokens, piece), cot_hbm=cotangent.reshape(chunks, tokens, piece),
        route_hbm=jnp.transpose(route_ids.reshape(chunks, tokens, 2), (0, 2, 1)),
        gain_hbm=norm_gain, router_hbm=router[0].T,
        w_gu=w_gate_up[0, 0], w_dn=w_down[0, 0],
    )
    outs = dict(
        rows=((chunks, cells, width), BF16), q=((chunks, cells, 2 * hidden_width), BF16),
        hidden=((chunks, cells, hidden_width), BF16), dy=((chunks, cells, width), BF16),
        gin=((chunks, tokens, piece), BF16), grad_router=((n_rank, width), F32),
        grad_gain=((1, width), F32),
    )
    exchanged = ((chunks, n_rank, blk, width), BF16)
    token_rows = ((chunks, tokens, width), BF16)
    line = ((chunks, n_rank, 1, LANES), F32)
    scratch = dict(
        x=((chunks, tokens, piece), BF16), cot=((chunks, tokens, piece), BF16),
        route=((chunks, 2, tokens), jnp.int32), gain=((1, width), F32),
        router_t=((n_rank, width), BF16),
        gu_buf=(w_gate_up[0, 0].shape, BF16), dn_buf=(w_down[0, 0].shape, BF16),
        rt=((2 * n_rank, width), BF16), acc=((n_rank, width), F32), gain_acc=((1, width), F32),
        tall=((chunks, tokens, LANES), F32), wide=((chunks, 8, tokens), F32),
        plain=((chunks, cells, hidden_width), F32), lean=((chunks, tokens, width), F32), cols=((chunks, tokens, 2 * n_rank), BF16),
        gain_out=((width // LANES, LANES), BF16), gain_land=((n_rank, width // LANES, LANES), BF16),
        ends=((chunks, n_sec, tokens, piece), BF16), fin=((chunks, n_sec - 1, tokens, piece), BF16),
        h=token_rows, u=token_rows, g=token_rows, h_out=token_rows, low=token_rows,
        keep=((chunks, tokens, LANES), F32), slope=((chunks, cells, 2 * hidden_width), F32),
        part_out=((n_rank, n_rank, part), BF16), part_land=((n_rank, n_rank, part), BF16),
        tot_out=((n_rank, part), BF16), tot_land=((n_rank, n_rank, part), BF16),
        u_out=exchanged, u_land=exchanged, y_out=exchanged, y_land=exchanged,
        g_out=exchanged, g_land=exchanged, du_out=exchanged, du_land=exchanged,
        gate_out=line, gate_land=line, dot_out=line, dot_land=line,
    )
    sems = dict(load_sem=(7,), send_sem=(KINDS, chunks), recv_sem=(KINDS, chunks), sum_sem=(6,))
    vmem = pl.BlockSpec(memory_space=pltpu.VMEM)
    hbm = pl.BlockSpec(memory_space=pltpu.HBM)
    cfg = (chunks, n_rank, n_dp, n_sec, tok, cap)
    made = pl.pallas_call(
        functools.partial(relay_body, cfg, list(args) + list(outs) + list(scratch) + list(sems)),
        out_shape=[pltpu.VMEM(*v) for v in outs.values()],
        in_specs=[hbm] * len(args),
        out_specs=[vmem] * len(outs),
        scratch_shapes=[pltpu.VMEM(*v) for v in scratch.values()]
        + [pltpu.SemaphoreType.DMA(v) for v in sems.values()],
        compiler_params=pltpu.CompilerParams(
            collective_id=1, has_side_effects=True, vmem_limit_bytes=LIMIT_RELAY * 1024 * 1024
        ),
    )(*args.values())
    made = types.SimpleNamespace(**dict(zip(outs, made)))

    def flat(value):
        return value.reshape(chunks * cells, -1)

    grad_gu, grad_dn, gin, grad_router, grad_gain = weight_grads(
        flat(made.rows), flat(made.q), flat(made.hidden), flat(made.dy),
        made.gin, made.grad_router, made.grad_gain,
    )
    return (
        gin.reshape(micro, tok, piece), grad_gu[None, None], grad_dn[None, None],
        grad_router.T[None], grad_gain,
    )


def solution(mesh):
    in_specs = (
        P(None, ("expert", "dp"), "section"),
        P(None, ("expert", "dp"), "section"),
        P("section", None, ("expert", "dp"), None),
        P("section", None),
        P("section", None, None),
        P("section", ("expert", "dp"), None, None),
        P("section", ("expert", "dp"), None, None),
    )
    out_specs = (
        P(None, ("expert", "dp"), "section"),
        P("section", ("expert", "dp"), None, None),
        P("section", ("expert", "dp"), None, None),
        P("section", None, None),
        P("section", None),
    )
    return jax.shard_map(local, mesh=mesh, in_specs=in_specs, out_specs=out_specs, check_vma=False)
```

```python
import functools
import types

import jax
import jax.numpy as jnp
from jax import lax
from jax.experimental import pallas as pl
from jax.experimental.pallas import tpu as pltpu
from jax.sharding import PartitionSpec as P

EPS = 1e-05
CHUNKS = 8
LANES = 128
WEIGHT_STEPS = 4
LIMIT_RELAY = 56
LIMIT_WEIGHT = 48
LAG_S = 5
LAG_F, LAG_T, LAG_B = (2, 3), (1, 2), (2, 4)
F32 = jnp.float32
BF16 = jnp.bfloat16
HIGH = lax.Precision.HIGHEST
ENDS, SEED, HX, GX, ROWS, GATE, BACK, TOP, DU, DOT, FIN = range(11)
KINDS = 11


def dot(a, b, dims, precision=None):
    return lax.dot_general(
        a, b, ((dims[:1], dims[1:]), ((), ())), precision=precision, preferred_element_type=F32
    )


def relay_body(cfg, names, *refs):
    r = types.SimpleNamespace(**dict(zip(names, refs)))
    chunks, n_rank, n_dp, n_sec, tok, cap = cfg
    _, tokens, piece = r.x.shape
    blk, width = r.u_land.shape[2:]
    cells = n_rank * blk
    hidden_width = r.w_dn.shape[0]
    n_expert = n_rank
    last = n_sec - 1
    section = lax.axis_index("section")
    me = lax.axis_index("expert") * n_dp + lax.axis_index("dp")
    send_sem, recv_sem = r.send_sem, r.recv_sem

    def place(step):
        rank = lax.rem(me + step, n_rank)
        return rank, {"expert": lax.div(rank, n_dp), "dp": lax.rem(rank, n_dp)}

    load_gu = pltpu.make_async_copy(r.w_gu, r.gu_buf, r.load_sem.at[0])
    load_dn = pltpu.make_async_copy(r.w_dn, r.dn_buf, r.load_sem.at[1])
    loads = [
        pltpu.make_async_copy(src, dst, r.load_sem.at[2 + i])
        for i, (src, dst) in enumerate((
            (r.x_hbm, r.x), (r.cot_hbm, r.cot), (r.route_hbm, r.route), (r.gain_hbm, r.gain),
            (r.router_hbm, r.router_t),
        ))
    ]
    for load in loads:
        load.start()
    load_gu.start()
    load_dn.start()
    barrier = pltpu.get_barrier_semaphore()
    for step in range(1, n_sec):
        pl.semaphore_signal(
            barrier, inc=1, device_id={"section": lax.rem(section + step, n_sec)},
            device_id_type=pl.DeviceIdType.MESH,
        )
    for step in range(1, n_rank):
        pl.semaphore_signal(
            barrier, inc=1, device_id=place(step)[1], device_id_type=pl.DeviceIdType.MESH
        )
    def iota(shape, axis):
        return lax.broadcasted_iota(jnp.int32, shape, axis)

    def loop(count, body):
        def run(t, carry):
            body(t)
            return carry

        lax.fori_loop(0, count, run, 0)

    def tabulate(c):
        route = r.route[c].astype(F32)
        rows, cols = iota((tokens, tokens), 0), iota((tokens, tokens), 1)
        eye = (rows == cols).astype(F32)
        early = ((lax.div(rows, tok) == lax.div(cols, tok)) & (cols < rows)).astype(F32)
        across = [route[k : k + 1, :] for k in range(2)]
        e = [jnp.sum(eye * v, axis=1, keepdims=True) for v in across]
        within = (lax.div(iota((tokens, 1), 0), tok) * cap).astype(F32)
        inner, cell = [], []
        for k in range(2):
            named = (across[0] == e[k]).astype(F32) + (across[1] == e[k]).astype(F32)
            inner.append(within + jnp.sum(early * named, axis=1, keepdims=True))
            cell.append(e[k] * blk + inner[k])
            r.wide[c, k : k + 1] = across[k]
            r.wide[c, 2 + k : 3 + k] = jnp.sum(eye * cell[k], axis=0, keepdims=True)
        at = iota((tokens, LANES), 1)
        tall = jnp.zeros((tokens, LANES), F32)
        for k, v in enumerate(e + inner + cell):
            tall = jnp.where(at == k, v, tall)
        r.tall[c] = tall

    pl.semaphore_wait(barrier, n_rank - 1 + n_sec - 1)
    for load in loads:
        load.wait()

    def push(src, dst, kind, c, device):
        pltpu.make_async_remote_copy(
            src_ref=src, dst_ref=dst, send_sem=send_sem.at[kind, c], recv_sem=recv_sem.at[kind, c],
            device_id=device, device_id_type=pl.DeviceIdType.MESH,
        ).start()

    for c in range(chunks):
        @pl.when(section > 0)
        def _():
            push(r.x.at[c], r.ends.at[c, section], ENDS, c, {"section": 0})

        @pl.when(section < last)
        def _():
            push(r.cot.at[c], r.ends.at[c, section], SEED, c, {"section": last})

    r.rt[:n_expert] = r.router_t[...]
    r.rt[n_expert:] = r.router_t[...]
    r.acc[...] = jnp.zeros(r.acc.shape, F32)
    r.gain_acc[...] = jnp.zeros(r.gain_acc.shape, F32)

    for c in range(chunks):
        tabulate(c)

    def spread(src, dst, kind, c):
        for step in range(1, n_rank):
            rank, device = place(step)
            push(src.at[rank], dst.at[me], kind, c, device)
        dst[me] = src[me]

    def settle(ref, sem):
        pltpu.make_async_copy(ref, ref, sem).wait()

    def landed(dst, kind, c):
        settle(dst.at[pl.ds(0, n_rank - 1)], recv_sem.at[kind, c])

    def sent(src, kind, c):
        settle(src.at[pl.ds(0, n_rank - 1)], send_sem.at[kind, c])

    def lanes_of(value):
        return value.reshape(n_rank, 1, LANES)

    lane_of_cell = lax.rem(iota((cells, LANES), 0), blk) == iota((cells, LANES), 1)
    lane_of_cell = lane_of_cell.astype(F32)

    def columns(c):
        tall = r.tall[c]
        e, inner, cell = ([tall[:, 2 * i + k : 2 * i + k + 1] for k in range(2)] for i in range(3))
        return e, inner, cell

    def to_cells(c):
        at = iota((cells, tokens), 0).astype(F32)
        return [(r.wide[c, 2 + k : 3 + k] == at).astype(F32) for k in range(2)]

    def from_cells(cell):
        at = iota((tokens, cells), 1).astype(F32)
        return [(cell[k] == at).astype(F32) for k in range(2)]

    def hits(e):
        at = iota((tokens, n_expert), 1).astype(F32)
        return [(e[k] == at).astype(F32) for k in range(2)]

    def slots(inner):
        at = iota((tokens, LANES), 1).astype(F32)
        return [(inner[k] == at).astype(F32) for k in range(2)]

    def dispatch(place_at, value, out, land, kind, c):
        rows = dot(place_at.astype(BF16), value, (1, 0)).astype(BF16)
        out[...] = rows.reshape(n_rank, blk, width)
        spread(out, land, kind, c)

    def signed(e, l):
        l_high = l.astype(BF16).astype(F32)
        at = iota((tokens, 2 * n_expert), 1)
        which = lax.rem(at, n_expert).astype(F32)
        signs = (e[0] == which).astype(F32) - (e[1] == which).astype(F32)
        return (jnp.where(at < n_expert, l_high, l - l_high) * signs).astype(BF16)

    def add_router(c, cols):
        term = dot(cols, r.u[c], (0, 0))
        r.acc[...] += term[:n_expert] + term[n_expert:]

    def send_tokens(c):
        @pl.when(section == 0)
        def _():
            settle(r.ends.at[c, pl.ds(0, n_sec - 1)], recv_sem.at[ENDS, c])
            r.h[c] = jnp.concatenate(
                [r.x[c]] + [r.ends[c, s] for s in range(1, n_sec)], axis=1
            )

        @pl.when(section > 0)
        def _():
            settle(r.h.at[c], recv_sem.at[HX, c])

        place_at = to_cells(c)
        h = r.h[c].astype(F32)
        inv = lax.rsqrt(jnp.mean(h * h, axis=-1, keepdims=True) + EPS)
        u = (h * inv * r.gain[...]).astype(BF16)
        dispatch(place_at[0] + place_at[1], u, r.u_out.at[c], r.u_land.at[c], ROWS, c)
        r.u[c] = u
        e, inner, _ = columns(c)
        hit = hits(e)
        diff = jnp.sum((hit[0] - hit[1]) * dot(u, r.router_t[...], (1, 1)), axis=1, keepdims=True)
        gate = [jax.nn.sigmoid(diff), jax.nn.sigmoid(-diff)]
        at = iota((tokens, LANES), 1)
        r.keep[c] = jnp.where(at == 0, gate[0], jnp.where(at == 1, gate[1], inv))

        @pl.when(section == last)
        def _():
            slot = slots(inner)
            at = iota((n_expert, tokens), 0).astype(F32)
            packed = sum(
                dot((r.wide[c, k : k + 1] == at).astype(F32), gate[k] * slot[k], (1, 0), HIGH)
                for k in range(2)
            )
            r.gate_out[c] = lanes_of(packed)
            spread(r.gate_out.at[c], r.gate_land.at[c], GATE, c)

    def expert_up(c):
        @pl.when(c == 0)
        def _():
            load_gu.wait()

        landed(r.u_land.at[c], ROWS, c)
        rows = r.u_land[c].reshape(cells, width)
        r.rows[c] = rows
        gate_up = dot(rows, r.gu_buf[...], (1, 0))
        a, b = gate_up[:, :hidden_width], gate_up[:, hidden_width:]
        sig = jax.nn.sigmoid(a)
        silu = a * sig
        hidden = (silu * b).astype(BF16)
        r.hidden[c] = hidden
        r.slope[c, :, :hidden_width] = b * (sig * (1.0 + a * (1.0 - sig)))
        r.slope[c, :, hidden_width:] = silu
        return hidden

    def expert_forward(c):
        hidden = expert_up(c)

        @pl.when(c == 0)
        def _():
            load_dn.wait()

        y = dot(hidden, r.dn_buf[...], (1, 0)).astype(BF16)
        r.y_out[c] = y.reshape(n_rank, blk, width)
        spread(r.y_out.at[c], r.y_land.at[c], BACK, c)

    def expert_down(c, d_hidden):
        slope = r.slope[c]
        q = jnp.concatenate(
            [d_hidden * slope[:, :hidden_width], d_hidden * slope[:, hidden_width:]], axis=1
        ).astype(BF16)
        r.q[c] = q
        du = dot(q, r.gu_buf[...], (1, 1)).astype(BF16)
        r.du_out[c] = du.reshape(n_rank, blk, width)
        spread(r.du_out.at[c], r.du_land.at[c], DU, c)
        both = r.rows[c].astype(F32) * du.astype(F32)
        r.gain_acc[...] += jnp.sum(both, axis=0, keepdims=True)

        @pl.when(c == chunks - 1)
        def _():
            r.gain_out[...] = jnp.concatenate(
                [r.gain_acc[:, i * LANES : (i + 1) * LANES] for i in range(lines)], axis=0
            ).astype(BF16)
            share_out(lambda rank: r.gain_out, r.gain_land, 2)

    def expert_backward(c):
        landed(r.g_land.at[c], TOP, c)
        top = r.g_land[c].reshape(cells, width)
        r.dy[c] = top
        expert_down(c, dot(top, r.dn_buf[...], (1, 1)))

    def expert_last(c):
        hidden = expert_up(c)
        landed(r.gate_land.at[c], GATE, c)
        spread_rows = (lax.div(iota((cells, n_rank), 0), blk) == iota((cells, n_rank), 1)).astype(F32)
        wide = dot(spread_rows, r.gate_land[c].reshape(n_rank, LANES), (1, 0), HIGH)
        gate = jnp.sum(wide * lane_of_cell, axis=1, keepdims=True)
        top = r.g_land[c].reshape(cells, width)
        plain = r.plain[c]
        expert_down(c, plain * gate)
        share = jnp.sum(plain * hidden.astype(F32), axis=1, keepdims=True)
        gather = (iota((n_rank, cells), 0) == lax.div(iota((n_rank, cells), 1), blk)).astype(F32)
        r.dot_out[c] = lanes_of(dot(gather, share * lane_of_cell, (1, 0), HIGH))
        spread(r.dot_out.at[c], r.dot_land.at[c], DOT, c)
        r.dy[c] = (top.astype(F32) * gate).astype(BF16)

    def combine_forward(c):
        pick = from_cells(columns(c)[2])
        keep = r.keep[c]
        landed(r.y_land.at[c], BACK, c)
        back = r.y_land[c].reshape(cells, width)
        picked = dot(jnp.concatenate(pick, axis=0).astype(BF16), back, (1, 0))
        h = r.h[c].astype(F32)
        up = h + keep[:, 0:1] * picked[:tokens] + keep[:, 1:2] * picked[tokens:]
        r.h_out[c] = up.astype(BF16)
        push(r.h_out.at[c], r.h.at[c], HX, c, {"section": section + 1})
        r.lean[c] = picked[:tokens] - picked[tokens:]

    def send_seed(c):
        settle(r.ends.at[c, pl.ds(0, n_sec - 1)], recv_sem.at[SEED, c])
        top = jnp.concatenate([r.ends[c, s] for s in range(last)] + [r.cot[c]], axis=1)
        r.g[c] = top
        place_at = to_cells(c)
        dispatch(place_at[0] + place_at[1], top, r.g_out.at[c], r.g_land.at[c], TOP, c)

    def expert_seed(c):
        @pl.when(c == 0)
        def _():
            load_dn.wait()

        landed(r.g_land.at[c], TOP, c)
        r.plain[c] = dot(r.g_land[c].reshape(cells, width), r.dn_buf[...], (1, 1))

    def send_top(c):
        place_at = jnp.concatenate(to_cells(c), axis=1)
        keep = r.keep[c]
        settle(r.g.at[c], recv_sem.at[GX, c])
        top = r.g[c].astype(F32)
        scaled = [(keep[:, k : k + 1] * top).astype(BF16) for k in range(2)]
        dispatch(
            place_at, jnp.concatenate(scaled, axis=0), r.g_out.at[c], r.g_land.at[c], TOP, c
        )
        share = jnp.sum(top * r.lean[c], axis=1, keepdims=True)
        cols = signed(columns(c)[0], keep[:, 0:1] * keep[:, 1:2] * share)
        r.cols[c] = cols
        add_router(c, cols)

        @pl.when(c == chunks - 1)
        def _():
            router_start()

    def finish_last(c):
        e, inner, cell = columns(c)
        hit, slot = hits(e), slots(inner)
        keep = r.keep[c]
        landed(r.dot_land.at[c], DOT, c)
        shares = r.dot_land[c].reshape(n_rank, LANES)
        wide = [dot(hit[k], shares, (1, 0), HIGH) * slot[k] for k in range(2)]
        share = jnp.sum(wide[0] - wide[1], axis=1, keepdims=True)
        cols = signed(e, keep[:, 0:1] * keep[:, 1:2] * share)
        finish(c, cols)
        add_router(c, cols)

    def finish(c, cols):
        pick = from_cells(columns(c)[2])
        inv = r.keep[c][:, 2:3]
        extra = dot(cols, r.rt[...], (1, 0))
        hn = r.h[c].astype(F32) * inv
        landed(r.du_land.at[c], DU, c)
        back = r.du_land[c].reshape(cells, width)
        du = dot((pick[0] + pick[1]).astype(BF16), back, (1, 0)) + extra
        scaled = du * r.gain[...]
        projection = jnp.mean(scaled * hn, axis=-1, keepdims=True)
        low = (r.g[c].astype(F32) + inv * (scaled - hn * projection)).astype(BF16)
        r.low[c] = low

        @pl.when(section > 0)
        def _():
            push(r.low.at[c], r.g.at[c], GX, c, {"section": section - 1})

        @pl.when(section == 0)
        def _():
            r.gin[c] = low[:, :piece]
            for s in range(1, n_sec):
                r.fin[c, s - 1] = low[:, s * piece : (s + 1) * piece]
                push(r.fin.at[c, s - 1], r.gin.at[c], FIN, c, {"section": s})

    part, lines = width // n_rank, width // LANES

    def share_out(src, dst, which):
        for step in range(1, n_rank):
            rank, device = place(step)
            pltpu.make_async_remote_copy(
                src_ref=src(rank), dst_ref=dst.at[me],
                send_sem=r.sum_sem.at[2 * which], recv_sem=r.sum_sem.at[2 * which + 1],
                device_id=device, device_id_type=pl.DeviceIdType.MESH,
            ).start()
        dst[me] = src(me)[...]

    def shared(dst, which, side):
        settle(dst.at[pl.ds(0, n_rank - 1)], r.sum_sem.at[2 * which + side])

    def router_start():
        for rank in range(n_rank):
            r.part_out[rank] = r.acc[:, rank * part : (rank + 1) * part].astype(BF16)
        share_out(lambda rank: r.part_out.at[rank], r.part_land, 0)

    def router_middle():
        shared(r.part_land, 0, 1)
        r.tot_out[...] = jnp.sum(r.part_land[...].astype(F32), axis=0).astype(BF16)
        share_out(lambda rank: r.tot_out, r.tot_land, 1)

    def guarded(t, body):
        @pl.when((t >= 0) & (t < chunks))
        def _():
            body(jnp.clip(t, 0, chunks - 1))

    def rounds(stages):
        def step(t):
            for lag, body in stages:
                guarded(t - lag, body)

        loop(chunks + max(lag for lag, _ in stages), step)

    @pl.when(section == last)
    def _():
        rounds(((0, send_seed), (LAG_S, expert_seed)))
        rounds(((0, send_tokens), (LAG_T[0], expert_last), (LAG_T[1], finish_last)))
        router_start()
        router_middle()

    @pl.when(section < last)
    def _():
        rounds(((0, send_tokens), (LAG_F[0], expert_forward), (LAG_F[1], combine_forward)))

        def middle(c):
            @pl.when(c == chunks - 1)
            def _():
                router_middle()

        rounds((
            (0, send_top), (LAG_B[0], expert_backward), (LAG_B[0], middle),
            (LAG_B[1], lambda c: finish(c, r.cols[c])),
        ))

    shared(r.tot_land, 1, 1)
    for rank in range(n_rank):
        r.grad_router[:, rank * part : (rank + 1) * part] = r.tot_land[rank].astype(F32)
    shared(r.gain_land, 2, 1)
    total = jnp.sum(r.gain_land[...].astype(F32), axis=0)
    routed = jnp.sum(r.router_t[...].astype(F32) * r.grad_router[...], axis=0, keepdims=True)
    for i in range(lines):
        lane = slice(i * LANES, (i + 1) * LANES)
        r.grad_gain[:, lane] = (total[i : i + 1] + routed[:, lane]) / r.gain[:, lane]
    shared(r.part_land, 0, 0)
    shared(r.tot_land, 1, 0)
    shared(r.gain_land, 2, 0)

    for c in range(chunks):
        for kind, ref in ((ROWS, r.u_out), (TOP, r.g_out), (DU, r.du_out)):
            sent(ref.at[c], kind, c)

        @pl.when(section == last)
        def _():
            sent(r.gate_out.at[c], GATE, c)
            sent(r.dot_out.at[c], DOT, c)

        @pl.when(section < last)
        def _():
            sent(r.y_out.at[c], BACK, c)
            settle(r.h_out.at[c], send_sem.at[HX, c])
            settle(r.cot.at[c], send_sem.at[SEED, c])

        @pl.when(section == 0)
        def _():
            settle(r.fin.at[c], send_sem.at[FIN, c])

        @pl.when(section > 0)
        def _():
            settle(r.x.at[c], send_sem.at[ENDS, c])
            settle(r.low.at[c], send_sem.at[GX, c])
            settle(r.gin.at[c], recv_sem.at[FIN, c])


def weight_body(steps, n_other, *refs):
    rows, q, hidden, dy = refs[:4]
    others = refs[4 : 4 + n_other]
    grad_gu, grad_dn = refs[4 + n_other : 6 + n_other]
    kept = refs[6 + n_other : 6 + 2 * n_other]
    up, down, sem = refs[6 + 2 * n_other :]
    writes = []
    for i in range(steps):
        for k, (buf, out, left, right) in enumerate(
            ((down, grad_dn, hidden, dy), (up, grad_gu, rows, q))
        ):
            size = buf.shape[0] // steps
            at = pl.ds(i * size, size)
            buf[at] = dot(left[:, at], right[...], (0, 0))
            write = pltpu.make_async_copy(buf.at[at], out.at[at], sem.at[k, i])
            write.start()
            writes.append(write)
    for given, copy in zip(others, kept):
        copy[...] = given[...]
    for write in writes:
        write.wait()


def weight_grads(rows, q, hidden, dy, *others):
    width, hidden_width = rows.shape[1], hidden.shape[1]
    shapes = [(width, 2 * hidden_width), (hidden_width, width)]
    vmem, hbm = pl.BlockSpec(memory_space=pltpu.VMEM), pl.BlockSpec(memory_space=pltpu.HBM)
    return pl.pallas_call(
        functools.partial(weight_body, WEIGHT_STEPS, len(others)),
        out_shape=[jax.ShapeDtypeStruct(v, F32) for v in shapes]
        + [jax.ShapeDtypeStruct(a.shape, a.dtype) for a in others],
        in_specs=[vmem] * (4 + len(others)),
        out_specs=[hbm] * 2 + [vmem] * len(others),
        scratch_shapes=[pltpu.VMEM(v, F32) for v in shapes]
        + [pltpu.SemaphoreType.DMA((2, WEIGHT_STEPS))],
        compiler_params=pltpu.CompilerParams(vmem_limit_bytes=LIMIT_WEIGHT * 1024 * 1024),
    )(rows, q, hidden, dy, *others)


def local(x_in, cotangent, route_ids, norm_gain, router, w_gate_up, w_down):
    micro, tok, piece = x_in.shape
    n_sec = lax.axis_size("section")
    n_dp = lax.axis_size("dp")
    n_rank = lax.axis_size("expert") * n_dp
    per_rank, hidden_width, width = w_down.shape[1:]
    assert per_rank == 1 and n_sec > 1
    cap = tok * 2 * 9 // (8 * n_rank)
    chunks = CHUNKS if micro % CHUNKS == 0 else 1
    per = micro // chunks
    tokens, blk = per * tok, per * cap
    cells = n_rank * blk
    part = width // n_rank
    args = dict(
        x_hbm=x_in.reshape(chunks, tokens, piece), cot_hbm=cotangent.reshape(chunks, tokens, piece),
        route_hbm=jnp.transpose(route_ids.reshape(chunks, tokens, 2), (0, 2, 1)),
        gain_hbm=norm_gain, router_hbm=router[0].T,
        w_gu=w_gate_up[0, 0], w_dn=w_down[0, 0],
    )
    outs = dict(
        rows=((chunks, cells, width), BF16), q=((chunks, cells, 2 * hidden_width), BF16),
        hidden=((chunks, cells, hidden_width), BF16), dy=((chunks, cells, width), BF16),
        gin=((chunks, tokens, piece), BF16), grad_router=((n_rank, width), F32),
        grad_gain=((1, width), F32),
    )
    exchanged = ((chunks, n_rank, blk, width), BF16)
    token_rows = ((chunks, tokens, width), BF16)
    line = ((chunks, n_rank, 1, LANES), F32)
    scratch = dict(
        x=((chunks, tokens, piece), BF16), cot=((chunks, tokens, piece), BF16),
        route=((chunks, 2, tokens), jnp.int32), gain=((1, width), F32),
        router_t=((n_rank, width), BF16),
        gu_buf=(w_gate_up[0, 0].shape, BF16), dn_buf=(w_down[0, 0].shape, BF16),
        rt=((2 * n_rank, width), BF16), acc=((n_rank, width), F32), gain_acc=((1, width), F32),
        tall=((chunks, tokens, LANES), F32), wide=((chunks, 8, tokens), F32),
        plain=((chunks, cells, hidden_width), F32), lean=((chunks, tokens, width), F32), cols=((chunks, tokens, 2 * n_rank), BF16),
        gain_out=((width // LANES, LANES), BF16), gain_land=((n_rank, width // LANES, LANES), BF16),
        ends=((chunks, n_sec, tokens, piece), BF16), fin=((chunks, n_sec - 1, tokens, piece), BF16),
        h=token_rows, u=token_rows, g=token_rows, h_out=token_rows, low=token_rows,
        keep=((chunks, tokens, LANES), F32), slope=((chunks, cells, 2 * hidden_width), F32),
        part_out=((n_rank, n_rank, part), BF16), part_land=((n_rank, n_rank, part), BF16),
        tot_out=((n_rank, part), BF16), tot_land=((n_rank, n_rank, part), BF16),
        u_out=exchanged, u_land=exchanged, y_out=exchanged, y_land=exchanged,
        g_out=exchanged, g_land=exchanged, du_out=exchanged, du_land=exchanged,
        gate_out=line, gate_land=line, dot_out=line, dot_land=line,
    )
    sems = dict(load_sem=(7,), send_sem=(KINDS, chunks), recv_sem=(KINDS, chunks), sum_sem=(6,))
    vmem = pl.BlockSpec(memory_space=pltpu.VMEM)
    hbm = pl.BlockSpec(memory_space=pltpu.HBM)
    cfg = (chunks, n_rank, n_dp, n_sec, tok, cap)
    made = pl.pallas_call(
        functools.partial(relay_body, cfg, list(args) + list(outs) + list(scratch) + list(sems)),
        out_shape=[pltpu.VMEM(*v) for v in outs.values()],
        in_specs=[hbm] * len(args),
        out_specs=[vmem] * len(outs),
        scratch_shapes=[pltpu.VMEM(*v) for v in scratch.values()]
        + [pltpu.SemaphoreType.DMA(v) for v in sems.values()],
        compiler_params=pltpu.CompilerParams(
            collective_id=1, has_side_effects=True, vmem_limit_bytes=LIMIT_RELAY * 1024 * 1024
        ),
    )(*args.values())
    made = types.SimpleNamespace(**dict(zip(outs, made)))

    def flat(value):
        return value.reshape(chunks * cells, -1)

    grad_gu, grad_dn, gin, grad_router, grad_gain = weight_grads(
        flat(made.rows), flat(made.q), flat(made.hidden), flat(made.dy),
        made.gin, made.grad_router, made.grad_gain,
    )
    return (
        gin.reshape(micro, tok, piece), grad_gu[None, None], grad_dn[None, None],
        grad_router.T[None], grad_gain,
    )


def solution(mesh):
    in_specs = (
        P(None, ("expert", "dp"), "section"),
        P(None, ("expert", "dp"), "section"),
        P("section", None, ("expert", "dp"), None),
        P("section", None),
        P("section", None, None),
        P("section", ("expert", "dp"), None, None),
        P("section", ("expert", "dp"), None, None),
    )
    out_specs = (
        P(None, ("expert", "dp"), "section"),
        P("section", ("expert", "dp"), None, None),
        P("section", ("expert", "dp"), None, None),
        P("section", None, None),
        P("section", None),
    )
    return jax.shard_map(local, mesh=mesh, in_specs=in_specs, out_specs=out_specs, check_vma=False)
```
